32 devices in a mesh: section: 8 (over z, x), tensor: 4 (over y, core).
Axes of the slice: x: 2, y: 2, z: 4, core: 2. Of those that a mesh axis runs over, the one named last changes fastest.
Arguments:
- hidden: bfloat16 [32, 8192], P(('section', 'tensor')), may hold values from -12 to 12
- weight: bfloat16 [16384, 8192], P(('section', 'tensor')), may hold values from -1 to 1
- targets: int32 [32], replicated, may hold values from 0 to 16383
- loss_grad: float32 [32], P(('section', 'tensor')), may hold values from 8 to 64
Outputs:
- token_loss: float32 [32], P(('section', 'tensor'))
- hidden_grad: bfloat16 [32, 8192], P(('section', 'tensor'))
The draws below stay inside these ranges and needn't reach their ends.
All inputs are finite; a program needn't handle non-finite values.
Results may differ from the reference program's by a relative error of at most 0.0039.
Values may be sent and summed in bfloat16 or wider, within the bound.
A program may use at most 64 MiB of HBM per device.

```python
import math
import jax
import jax.numpy as jnp
from jax import lax

D = 8192
TOKENS = 32
VOCAB = 16384


def weight_matrix(key):
    base_key = jax.random.fold_in(key, 11)
    keys = jax.random.split(base_key, 1)
    ramp = 1.0 + 0.25 * jnp.arange(VOCAB, dtype=jnp.float32) / VOCAB
    entries = jax.random.truncated_normal(keys[0], -6.0, 6.0, (VOCAB, D), jnp.float32)
    return (entries * ramp[:, None] * (3.0 / math.sqrt(D))).astype(jnp.bfloat16)


def draw_weight(key, part):
    return weight_matrix(key)


def draw_hidden(key, part):
    keys = jax.random.split(jax.random.fold_in(key, 23), 1)
    limit = 12.0 * max(1, 512 // D)
    values = jax.random.truncated_normal(keys[0], -6.0, 6.0, (TOKENS, D), jnp.float32)
    values = jnp.clip(values, -limit, limit)
    return values.astype(jnp.bfloat16)


def place_ends(array, stream_key, least, high):
    longest = array.shape.index(max(array.shape))
    spots = []
    for shift in (0, 1):
        where = [jax.random.randint(jax.random.fold_in(stream_key, axis), (), 0, length) for axis, length in enumerate(array.shape)]
        where[longest] = (where[longest] + shift) % array.shape[longest]
        spots.append(tuple(where))
    return array.at[spots[0]].set(least).at[spots[1]].set(high)


def steps_of(stream_key, dims, cuts, smallest, high):
    def one(dim, blocks):
        steps = jax.random.uniform(jax.random.fold_in(jax.random.fold_in(stream_key, 6), dim), (blocks,), jnp.float32, smallest / len(cuts), high / len(cuts))
        return jnp.repeat(jnp.exp(steps), dims[dim] // blocks).reshape((-1,) + (1,) * (len(dims) - dim - 1))

    level = one(*cuts[0])
    for cut in cuts[1:]:
        level = level * one(*cut)
    return level


def setup_inputs(seed: int = 0) -> dict:
    arg_keys = jax.random.split(jax.random.key(seed), 5)
    return {
        "hidden": draw_hidden(jax.random.fold_in(arg_keys[4], 71), 0),
        "weight": draw_weight(jax.random.fold_in(arg_keys[4], 71), 0),
        "targets": place_ends(jax.random.randint(arg_keys[2], (TOKENS,), 0, VOCAB), jax.random.fold_in(arg_keys[2], 1), 0, VOCAB - 1).astype(jnp.int32),
        "loss_grad": jnp.clip(jnp.exp(math.log(64.0) - 2.0794415 * jax.random.uniform(arg_keys[3], (TOKENS,), jnp.float32) ** steps_of(arg_keys[3], (TOKENS,), ((0, 32),), -0.2, 0.2)), 8.0, 64.0),
    }


def reference(hidden, weight, targets, loss_grad):
    logits = lax.dot_general(hidden, weight, (((1,), (1,)), ((), ())), preferred_element_type=jnp.float32)
    row_max = jnp.max(logits, axis=1)
    shifted = jnp.exp(logits - row_max[:, None])
    exp_total = jnp.sum(shifted, axis=1)
    target_logit = jnp.take_along_axis(logits, targets[:, None].astype(jnp.int32), axis=1)[:, 0]
    token_loss = row_max + jnp.log(exp_total) - target_logit
    columns = lax.broadcasted_iota(jnp.int32, logits.shape, 1)
    one_hot = (columns == targets[:, None].astype(jnp.int32)).astype(jnp.float32)
    probs_grad = (shifted / exp_total[:, None] - one_hot).astype(jnp.bfloat16)
    grad_sum = jnp.dot(probs_grad, weight, preferred_element_type=jnp.float32)
    hidden_grad = (loss_grad[:, None] * grad_sum).astype(jnp.bfloat16)
    return (token_loss, hidden_grad)
```

```python
import functools

import jax
import jax.numpy as jnp
from jax import lax
from jax.experimental import pallas as pl
from jax.experimental.pallas import tpu as pltpu
from jax.sharding import PartitionSpec as P

MESH = pl.DeviceIdType.MESH
LANES = 128
GROUP = 8


def kernel(S, T, hid_ref, w_hbm, tgt_ref, lg_ref, loss_ref, out_ref,
           wv, hbuf, slab, gt, sendbuf, rbuf, rowbuf, st_send, st_recv,
           w_sem, ag_send, ag_recv, st_ssem, st_rsem, rs_send, rs_recv):
    n = S * T
    H = T // 2
    V, D = wv.shape
    C = D // LANES
    L = st_send.shape[2]
    s = lax.axis_index("section")
    t = lax.axis_index("tensor")
    me = s * T + t
    pt = t + 1 - 2 * lax.rem(t, 2)

    def sec(k):
        return lax.rem(s + k + S, S)

    def ten(j):
        return lax.rem(t + 2 * j + T, T)

    parts = w_sem.shape[0]
    rows = V // parts

    def w_copy(q):
        r = pl.ds(q * rows, rows)
        return pltpu.make_async_copy(w_hbm.at[r], wv.at[r], w_sem.at[q])

    for q in range(parts):
        w_copy(q).start()

    barrier = pltpu.get_barrier_semaphore()

    def greet(k, _):
        o = lax.rem(me + k, n)
        pl.semaphore_signal(barrier, inc=1, device_id=(o // T, lax.rem(o, T)), device_id_type=MESH)
        return 0

    lax.fori_loop(1, n, greet, 0)

    own = hid_ref[...].astype(jnp.float32)
    for c in range(C):
        rowbuf[c:c + 1, :] = own[:, c * LANES:(c + 1) * LANES]
    hbuf[me] = rowbuf[...].astype(jnp.bfloat16)

    pl.semaphore_wait(barrier, n - 1)

    def ag(tok, ds, dt):
        pltpu.make_async_remote_copy(
            src_ref=hbuf.at[tok], dst_ref=hbuf.at[tok], send_sem=ag_send,
            recv_sem=ag_recv.at[tok], device_id=(ds, dt), device_id_type=MESH).start()

    def landed(buf, sem, i):
        pltpu.make_async_copy(buf.at[i], buf.at[i], sem.at[i]).wait()

    def forward(tok):
        for j in range(1, H):
            ag(tok, s, ten(j))
        ag(tok, s, pt)

    def p1(k, _):
        ag(me, sec(k), t)
        return 0

    lax.fori_loop(1, S, p1, 0)
    forward(me)

    def p2(k, _):
        tok = sec(-k) * T + t
        landed(hbuf, ag_recv, tok)
        forward(tok)
        return 0

    lax.fori_loop(1, S, p2, 0)
    for j in range(1, H):
        def p3(k, _, j=j):
            tok = sec(-k) * T + ten(-j)
            landed(hbuf, ag_recv, tok)
            ag(tok, s, pt)
            return 0

        lax.fori_loop(0, S, p3, 0)

    tcol = lax.fori_loop(
        0, n, lambda i, x: jnp.where(lax.broadcasted_iota(jnp.int32, (n, LANES), 0) == i, tgt_ref[i], x),
        jnp.zeros((n, LANES), jnp.int32))[:, :1]

    for j in range(H):
        def p4(k, _, j=j):
            tok = sec(-k) * T + lax.rem(pt + 2 * j, T)
            landed(hbuf, ag_recv, tok)
            return 0

        lax.fori_loop(0, S, p4, 0)

    def widen(i, _):
        slab[pl.ds(pl.multiple_of(i * C, C), C), :] = hbuf[i].astype(jnp.float32)
        return 0

    lax.fori_loop(0, n, widen, 0)
    for q in range(parts):
        w_copy(q).wait()

    KC = GROUP * LANES

    def dot1(kc, acc):
        lhs = jnp.concatenate(
            [slab[pl.ds(kc * GROUP + i, n, stride=C), :] for i in range(GROUP)], axis=1).astype(jnp.bfloat16)
        w = wv[:, pl.ds(pl.multiple_of(kc * KC, KC), KC)]
        return acc + lax.dot_general(lhs, w, (((1,), (1,)), ((), ())), preferred_element_type=jnp.float32)

    logits = lax.fori_loop(0, D // KC, dot1, jnp.zeros((n, V), jnp.float32))

    mask = lax.broadcasted_iota(jnp.int32, (n, V), 1) + me * V == tcol
    m = jnp.max(logits, axis=1, keepdims=True)
    e = jnp.exp(logits - m)
    total = jnp.sum(e, axis=1, keepdims=True)
    tl = jnp.sum(jnp.where(mask, logits, 0.0), axis=1, keepdims=True)
    ptl = jnp.sum(jnp.where(mask, e, 0.0), axis=1, keepdims=True)

    r = lax.broadcasted_iota(jnp.int32, (n, L), 0)
    c = lax.broadcasted_iota(jnp.int32, (n, L), 1)
    packed = jnp.where(c == r, m, jnp.where(c == r + n, total, jnp.where(c == r + 2 * n, tl, 0.0)))
    packed = jnp.sum(packed, axis=0, keepdims=True)
    st_send[0] = packed
    st_recv[0] = packed

    def share(k, _):
        o = lax.rem(me + k, n)
        pltpu.make_async_remote_copy(
            src_ref=st_send.at[0], dst_ref=st_recv.at[k], send_sem=st_ssem, recv_sem=st_rsem,
            device_id=(o // T, lax.rem(o, T)), device_id_type=MESH).start()
        return 0

    lax.fori_loop(1, n, share, 0)

    lhs2 = jnp.concatenate(
        [jnp.where(mask, 0.0, e), mask.astype(jnp.float32)], axis=0).astype(jnp.bfloat16)

    def dot2(kc, _):
        cols = pl.ds(pl.multiple_of(kc * KC, KC), KC)
        gt[:, cols] = jnp.dot(lhs2, wv[:, cols], preferred_element_type=jnp.float32)
        return 0

    lax.fori_loop(0, D // KC, dot2, 0)

    others = st_recv.at[pl.ds(1, n - 1)]
    pltpu.make_async_copy(others, others, st_rsem).wait()

    top = lax.fori_loop(1, n, lambda k, x: jnp.maximum(x, st_recv[k]), st_recv[0])

    lane = lax.broadcasted_iota(jnp.int32, (1, L), 1)
    live = lane < n
    top = jnp.where(live, top, 0.0)

    def add_live(k, carry):
        z, g = carry
        row = st_recv[k]
        gap = jnp.where(live, row - top, 0.0)
        return z + jnp.exp(gap) * pltpu.roll(row, L - n, 1), g + pltpu.roll(row, L - 2 * n, 1)

    z, g = lax.fori_loop(0, n, add_live, (jnp.zeros((1, L), jnp.float32), jnp.zeros((1, L), jnp.float32)))
    z = jnp.where(live, z, 1.0)
    loss_ref[0] = jnp.sum(jnp.where(lane == me, top + jnp.log(z) - g, 0.0))
    top_c = jnp.sum(jnp.where(c == r, top, 0.0), axis=1, keepdims=True)
    z_c = jnp.sum(jnp.where(c == r, z, 0.0), axis=1, keepdims=True)
    scale = jnp.exp(m - top_c) / z_c
    hit = ptl * scale - 1.0

    def spread(kc, _):
        for i in range(GROUP):
            cols = pl.ds(pl.multiple_of(kc * KC + i * LANES, LANES), LANES)
            slab[pl.ds(kc * GROUP + i, n, stride=C), :] = scale * gt[:n, cols] + hit * gt[n:, cols]
        return 0

    lax.fori_loop(0, D // KC, spread, 0)

    def part(tok):
        return slab[pl.ds(pl.multiple_of(tok * C, C), C), :]

    def rs(tok, slot, value, ds, dt):
        sendbuf[tok] = value.astype(jnp.bfloat16)
        pltpu.make_async_remote_copy(
            src_ref=sendbuf.at[tok], dst_ref=rbuf.at[slot], send_sem=rs_send,
            recv_sem=rs_recv.at[slot], device_id=(ds, dt), device_id_type=MESH).start()

    def got(slot):
        landed(rbuf, rs_recv, slot)
        return rbuf[slot].astype(jnp.float32)

    for j in [*range(1, H), 0]:
        def qa(k, _, j=j):
            tok = sec(k + 1) * T + lax.rem(pt + 2 * j, T)
            rs(tok, tok, part(tok), s, pt)
            return 0

        lax.fori_loop(0, S, qa, 0)

    for j in range(1, H):
        def qb(k, _, j=j):
            tp = ten(j)
            sp = sec(k + 1)
            tok = sp * T + tp
            rs(tok, sp * T + pt, part(tok) + got(tok), s, tp)
            return 0

        lax.fori_loop(0, S, qb, 0)

    def joined(sp):
        tok = sp * T + t
        acc = part(tok) + got(tok)
        for j in range(1, H):
            acc = acc + got(sp * T + lax.rem(pt + 2 * j, T))
        return acc

    def qc(k, _):
        sp = sec(k)
        rs(sp * T + t, s * T + pt, joined(sp), sp, t)
        return 0

    lax.fori_loop(1, S, qc, 0)
    mine = lax.fori_loop(1, S, lambda k, x: x + got(sec(-k) * T + pt), joined(s))
    out_ref[...] = (lg_ref[0] * mine).astype(jnp.bfloat16)

    sent = hbuf.at[pl.ds(0, n - 1)]
    pltpu.make_async_copy(sent, sent, ag_send).wait()
    pltpu.make_async_copy(others, others, st_ssem).wait()
    sent = sendbuf.at[pl.ds(0, n - 1)]
    pltpu.make_async_copy(sent, sent, rs_send).wait()


def solution(mesh):
    S, T = mesh.shape["section"], mesh.shape["tensor"]
    n = S * T

    def step(hidden, weight, targets, loss_grad):
        V, D = weight.shape
        C = D // LANES
        L = -(-3 * n // LANES) * LANES
        vmem, smem = pltpu.VMEM, pltpu.SMEM
        loss, grad = pl.pallas_call(
            functools.partial(kernel, S, T),
            out_shape=(
                jax.ShapeDtypeStruct((1,), jnp.float32),
                jax.ShapeDtypeStruct((C, LANES), jnp.bfloat16),
            ),
            in_specs=[
                pl.BlockSpec(memory_space=vmem),
                pl.BlockSpec(memory_space=pl.ANY),
                pl.BlockSpec(memory_space=smem),
                pl.BlockSpec(memory_space=smem),
            ],
            out_specs=(pl.BlockSpec(memory_space=smem), pl.BlockSpec(memory_space=vmem)),
            scratch_shapes=[
                vmem((V, D), jnp.bfloat16),
                vmem((n, C, LANES), jnp.bfloat16),
                vmem((n * C, LANES), jnp.float32),
                vmem((2 * n, D), jnp.float32),
                vmem((n, C, LANES), jnp.bfloat16),
                vmem((n, C, LANES), jnp.bfloat16),
                vmem((C, LANES), jnp.float32),
                vmem((1, 1, L), jnp.float32),
                vmem((n, 1, L), jnp.float32),
                pltpu.SemaphoreType.DMA((4,)),
                pltpu.SemaphoreType.DMA,
                pltpu.SemaphoreType.DMA((n,)),
                pltpu.SemaphoreType.DMA,
                pltpu.SemaphoreType.DMA,
                pltpu.SemaphoreType.DMA,
                pltpu.SemaphoreType.DMA((n,)),
            ],
            compiler_params=pltpu.CompilerParams(
                collective_id=0, has_side_effects=True, vmem_limit_bytes=67043328
            ),
        )(hidden, weight, targets, loss_grad)
        return loss, grad.reshape(1, D)

    return jax.shard_map(
        step,
        mesh=mesh,
        in_specs=(
            P(("section", "tensor"), None),
            P(("section", "tensor"), None),
            P(),
            P(("section", "tensor")),
        ),
        out_specs=(P(("section", "tensor")), P(("section", "tensor"), None)),
        check_vma=False,
    )
```

```python
import functools

import jax
import jax.numpy as jnp
from jax import lax
from jax.experimental import pallas as pl
from jax.experimental.pallas import tpu as pltpu
from jax.sharding import PartitionSpec as P

MESH = pl.DeviceIdType.MESH
LANES = 128
GROUP = 8


def kernel(S, T, hid_hbm, w_hbm, tgt_hbm, lg_hbm, loss_ref, out_ref,
           hid_ref, tgt_ref, lg_ref, in_sem,
           wv, hbuf, slab, gt, sendbuf, rbuf, rowbuf, st_send, st_recv,
           w_sem, ag_send, ag_recv, st_ssem, st_rsem, rs_send, rs_recv):
    n = S * T
    H = T // 2
    V, D = wv.shape
    C = D // LANES
    pitch = C + 8
    L = st_send.shape[2]
    s = lax.axis_index("section")
    t = lax.axis_index("tensor")
    me = s * T + t
    pt = t + 1 - 2 * lax.rem(t, 2)

    def sec(k):
        return lax.rem(s + k + S, S)

    def ten(j):
        return lax.rem(t + 2 * j + T, T)

    parts = w_sem.shape[0]
    rows = V // parts

    def w_copy(q):
        r = pl.ds(q * rows, rows)
        return pltpu.make_async_copy(w_hbm.at[r], wv.at[r], w_sem.at[q])

    barrier = pltpu.get_barrier_semaphore()

    def greet(k, _):
        o = lax.rem(me + k, n)
        pl.semaphore_signal(barrier, inc=1, device_id=(o // T, lax.rem(o, T)), device_id_type=MESH)
        return 0

    lax.fori_loop(1, n, greet, 0)

    hid_copy = pltpu.make_async_copy(hid_hbm, hid_ref, in_sem.at[0])
    tgt_copy = pltpu.make_async_copy(tgt_hbm, tgt_ref, in_sem.at[1])
    lg_copy = pltpu.make_async_copy(lg_hbm, lg_ref, in_sem.at[2])
    hid_copy.start()
    tgt_copy.start()
    lg_copy.start()
    for q in range(parts):
        w_copy(q).start()
    hid_copy.wait()
    own = hid_ref[...].astype(jnp.float32)
    for c in range(C):
        rowbuf[c:c + 1, :] = own[:, c * LANES:(c + 1) * LANES]
    hbuf[me] = rowbuf[...].astype(jnp.bfloat16)

    pl.semaphore_wait(barrier, n - 1)

    def ag(tok, ds, dt):
        pltpu.make_async_remote_copy(
            src_ref=hbuf.at[tok], dst_ref=hbuf.at[tok], send_sem=ag_send,
            recv_sem=ag_recv.at[tok], device_id=(ds, dt), device_id_type=MESH).start()

    def landed(buf, sem, i):
        pltpu.make_async_copy(buf.at[i], buf.at[i], sem.at[i]).wait()

    def forward(tok):
        for j in range(1, H):
            ag(tok, s, ten(j))
        ag(tok, s, pt)

    def p1(k, _):
        ag(me, sec(k), t)
        return 0

    lax.fori_loop(1, S, p1, 0)
    forward(me)

    def p2(k, _):
        tok = sec(-k) * T + t
        landed(hbuf, ag_recv, tok)
        forward(tok)
        return 0

    lax.fori_loop(1, S, p2, 0)
    for j in range(1, H):
        def p3(k, _, j=j):
            tok = sec(-k) * T + ten(-j)
            landed(hbuf, ag_recv, tok)
            ag(tok, s, pt)
            return 0

        lax.fori_loop(0, S, p3, 0)

    tgt_copy.wait()
    lg_copy.wait()
    tcol = lax.fori_loop(
        0, n, lambda i, x: jnp.where(lax.broadcasted_iota(jnp.int32, (n, LANES), 0) == i, tgt_ref[i], x),
        jnp.zeros((n, LANES), jnp.int32))[:, :1]

    for j in range(H):
        def p4(k, _, j=j):
            tok = sec(-k) * T + lax.rem(pt + 2 * j, T)
            landed(hbuf, ag_recv, tok)
            return 0

        lax.fori_loop(0, S, p4, 0)

    def widen(i, _):
        slab[pl.ds(pl.multiple_of(i * pitch, 8), C), :] = hbuf[i].astype(jnp.float32)
        return 0

    lax.fori_loop(0, n, widen, 0)
    for q in range(parts):
        w_copy(q).wait()

    KC = GROUP * LANES

    def dot1(kc, acc):
        lhs = jnp.concatenate(
            [slab[pl.ds(kc * GROUP + i, n, stride=pitch), :] for i in range(GROUP)], axis=1).astype(jnp.bfloat16)
        w = wv[:, pl.ds(pl.multiple_of(kc * KC, KC), KC)]
        return acc + lax.dot_general(lhs, w, (((1,), (1,)), ((), ())), preferred_element_type=jnp.float32)

    logits = lax.fori_loop(0, D // KC, dot1, jnp.zeros((n, V), jnp.float32))

    mask = lax.broadcasted_iota(jnp.int32, (n, V), 1) + me * V == tcol
    m = jnp.max(logits, axis=1, keepdims=True)
    e = jnp.exp(logits - m)
    total = jnp.sum(e, axis=1, keepdims=True)
    tl = jnp.sum(jnp.where(mask, logits, 0.0), axis=1, keepdims=True)
    ptl = jnp.sum(jnp.where(mask, e, 0.0), axis=1, keepdims=True)

    r = lax.broadcasted_iota(jnp.int32, (n, L), 0)
    c = lax.broadcasted_iota(jnp.int32, (n, L), 1)
    packed = jnp.where(c == r, m, jnp.where(c == r + n, total, jnp.where(c == r + 2 * n, tl, 0.0)))
    packed = jnp.sum(packed, axis=0, keepdims=True)
    st_send[0] = packed
    st_recv[0] = packed

    def share(k, _):
        o = lax.rem(me + k, n)
        pltpu.make_async_remote_copy(
            src_ref=st_send.at[0], dst_ref=st_recv.at[k], send_sem=st_ssem, recv_sem=st_rsem,
            device_id=(o // T, lax.rem(o, T)), device_id_type=MESH).start()
        return 0

    lax.fori_loop(1, n, share, 0)

    lhs2 = jnp.concatenate(
        [jnp.where(mask, 0.0, e), mask.astype(jnp.float32)], axis=0).astype(jnp.bfloat16)

    def dot2(kc, _):
        cols = pl.ds(pl.multiple_of(kc * KC, KC), KC)
        gt[:, cols] = jnp.dot(lhs2, wv[:, cols], preferred_element_type=jnp.float32)
        return 0

    lax.fori_loop(0, D // KC, dot2, 0)

    others = st_recv.at[pl.ds(1, n - 1)]
    pltpu.make_async_copy(others, others, st_rsem).wait()

    lane = lax.broadcasted_iota(jnp.int32, (1, L), 1)
    live = lane < n
    got_stats = st_recv[...]
    top = jnp.where(live, jnp.max(got_stats, axis=0), 0.0)
    gap = jnp.where(live[None], got_stats - top[None], 0.0)
    z = jnp.sum(jnp.exp(gap) * pltpu.roll(got_stats, L - n, 2), axis=0)
    g = pltpu.roll(jnp.sum(got_stats, axis=0), L - 2 * n, 1)
    z = jnp.where(live, z, 1.0)
    loss_ref[0] = jnp.sum(jnp.where(lane == me, top + jnp.log(z) - g, 0.0))
    top_c = jnp.sum(jnp.where(c == r, top, 0.0), axis=1, keepdims=True)
    z_c = jnp.sum(jnp.where(c == r, z, 0.0), axis=1, keepdims=True)
    scale = jnp.exp(m - top_c) / z_c
    hit = ptl * scale - 1.0

    def spread(kc, _):
        for i in range(GROUP):
            cols = pl.ds(pl.multiple_of(kc * KC + i * LANES, LANES), LANES)
            slab[pl.ds(kc * GROUP + i, n, stride=pitch), :] = scale * gt[:n, cols] + hit * gt[n:, cols]
        return 0

    lax.fori_loop(0, D // KC, spread, 0)

    def part(tok):
        return slab[pl.ds(pl.multiple_of(tok * pitch, 8), C), :]

    def rs(tok, slot, value, ds, dt):
        sendbuf[tok] = value.astype(jnp.bfloat16)
        pltpu.make_async_remote_copy(
            src_ref=sendbuf.at[tok], dst_ref=rbuf.at[slot], send_sem=rs_send,
            recv_sem=rs_recv.at[slot], device_id=(ds, dt), device_id_type=MESH).start()

    def got(slot):
        landed(rbuf, rs_recv, slot)
        return rbuf[slot].astype(jnp.float32)

    for j in [*range(1, H), 0]:
        def qa(k, _, j=j):
            tok = sec(k + 1) * T + lax.rem(pt + 2 * j, T)
            rs(tok, tok, part(tok), s, pt)
            return 0

        lax.fori_loop(0, S, qa, 0)

    for j in range(1, H):
        def qb(k, _, j=j):
            tp = ten(j)
            sp = sec(k + 1)
            tok = sp * T + tp
            rs(tok, sp * T + pt, part(tok) + got(tok), s, tp)
            return 0

        lax.fori_loop(0, S, qb, 0)

    def joined(sp):
        tok = sp * T + t
        acc = part(tok) + got(tok)
        for j in range(1, H):
            acc = acc + got(sp * T + lax.rem(pt + 2 * j, T))
        return acc

    def qc(k, _):
        sp = sec(k)
        rs(sp * T + t, s * T + pt, joined(sp), sp, t)
        return 0

    lax.fori_loop(1, S, qc, 0)
    mine = lax.fori_loop(1, S, lambda k, x: x + got(sec(-k) * T + pt), joined(s))
    out_ref[...] = (lg_ref[0] * mine).astype(jnp.bfloat16)

    sent = hbuf.at[pl.ds(0, n - 1)]
    pltpu.make_async_copy(sent, sent, ag_send).wait()
    pltpu.make_async_copy(others, others, st_ssem).wait()
    sent = sendbuf.at[pl.ds(0, n - 1)]
    pltpu.make_async_copy(sent, sent, rs_send).wait()


def solution(mesh):
    S, T = mesh.shape["section"], mesh.shape["tensor"]
    n = S * T

    def step(hidden, weight, targets, loss_grad):
        V, D = weight.shape
        C = D // LANES
        L = -(-3 * n // LANES) * LANES
        vmem, smem = pltpu.VMEM, pltpu.SMEM
        loss, grad = pl.pallas_call(
            functools.partial(kernel, S, T),
            out_shape=(
                jax.ShapeDtypeStruct((1,), jnp.float32),
                jax.ShapeDtypeStruct((C, LANES), jnp.bfloat16),
            ),
            in_specs=[
                pl.BlockSpec(memory_space=pl.ANY)
            ] * 4,
            out_specs=(pl.BlockSpec(memory_space=smem), pl.BlockSpec(memory_space=vmem)),
            scratch_shapes=[
                vmem((1, D), jnp.bfloat16),
                smem((n,), jnp.int32),
                smem((1,), jnp.float32),
                pltpu.SemaphoreType.DMA((3,)),
                vmem((V, D), jnp.bfloat16),
                vmem((n, C, LANES), jnp.bfloat16),
                vmem((n * (C + 8), LANES), jnp.float32),
                vmem((2 * n, D), jnp.float32),
                vmem((n, C, LANES), jnp.bfloat16),
                vmem((n, C, LANES), jnp.bfloat16),
                vmem((C, LANES), jnp.float32),
                vmem((1, 1, L), jnp.float32),
                vmem((n, 1, L), jnp.float32),
                pltpu.SemaphoreType.DMA((4,)),
                pltpu.SemaphoreType.DMA,
                pltpu.SemaphoreType.DMA((n,)),
                pltpu.SemaphoreType.DMA,
                pltpu.SemaphoreType.DMA,
                pltpu.SemaphoreType.DMA,
                pltpu.SemaphoreType.DMA((n,)),
            ],
            compiler_params=pltpu.CompilerParams(
                collective_id=0, has_side_effects=True, vmem_limit_bytes=67043328
            ),
        )(hidden, weight, targets, loss_grad)
        return loss, grad.reshape(1, D)

    return jax.shard_map(
        step,
        mesh=mesh,
        in_specs=(
            P(("section", "tensor"), None),
            P(("section", "tensor"), None),
            P(),
            P(("section", "tensor")),
        ),
        out_specs=(P(("section", "tensor")), P(("section", "tensor"), None)),
        check_vma=False,
    )
```

```python
import functools
import math

import jax
import jax.numpy as jnp
from jax import lax
from jax.experimental import pallas as pl
from jax.experimental.pallas import tpu as pltpu
from jax.sharding import PartitionSpec as P

MESH = pl.DeviceIdType.MESH
LANES = 128
GROUP = 8
WIDE = 32


def kernel(S, T, hid_hbm, w_hbm, tgt_hbm, lg_hbm, loss_ref, out_ref,
           hid_ref, tgt_ref, lg_ref, in_sem,
           wv, hbuf, slab, gt, sendbuf, rbuf, rowbuf, st_send, st_recv,
           w_sem, ag_send, ag_recv, st_ssem, st_rsem, rs_send, rs_recv):
    n = S * T
    H = T // 2
    V, D = wv.shape
    C = D // LANES
    pitch = C + 8
    L = st_send.shape[2]
    s = lax.axis_index("section")
    t = lax.axis_index("tensor")
    me = s * T + t
    pt = t + 1 - 2 * lax.rem(t, 2)

    def sec(k):
        return lax.rem(s + k + S, S)

    def ten(j):
        return lax.rem(t + 2 * j + T, T)

    parts = w_sem.shape[0]
    rows = V // parts

    def w_copy(q):
        r = pl.ds(q * rows, rows)
        return pltpu.make_async_copy(w_hbm.at[r], wv.at[r], w_sem.at[q])

    barrier = pltpu.get_barrier_semaphore()

    def greet(k, _):
        o = lax.rem(me + k, n)
        pl.semaphore_signal(barrier, inc=1, device_id=(o // T, lax.rem(o, T)), device_id_type=MESH)
        return 0

    lax.fori_loop(1, n, greet, 0)

    hid_copy = pltpu.make_async_copy(hid_hbm, hid_ref, in_sem.at[0])
    tgt_copy = pltpu.make_async_copy(tgt_hbm, tgt_ref, in_sem.at[1])
    lg_copy = pltpu.make_async_copy(lg_hbm, lg_ref, in_sem.at[2])
    hid_copy.start()
    tgt_copy.start()
    lg_copy.start()
    for q in range(parts):
        w_copy(q).start()
    hid_copy.wait()
    own = hid_ref[...].astype(jnp.float32)
    for c in range(C):
        rowbuf[c:c + 1, :] = own[:, c * LANES:(c + 1) * LANES]
    hbuf[me] = rowbuf[...].astype(jnp.bfloat16)

    pl.semaphore_wait(barrier, n - 1)

    def ag(tok, ds, dt):
        pltpu.make_async_remote_copy(
            src_ref=hbuf.at[tok], dst_ref=hbuf.at[tok], send_sem=ag_send,
            recv_sem=ag_recv.at[tok], device_id=(ds, dt), device_id_type=MESH).start()

    def landed(buf, sem, i):
        pltpu.make_async_copy(buf.at[i], buf.at[i], sem.at[i]).wait()

    def forward(tok):
        for j in range(1, H):
            ag(tok, s, ten(j))
        ag(tok, s, pt)

    def p1(k, _):
        ag(me, sec(k), t)
        return 0

    lax.fori_loop(1, S, p1, 0)
    forward(me)

    def p2(k, _):
        tok = sec(-k) * T + t
        landed(hbuf, ag_recv, tok)
        forward(tok)
        return 0

    lax.fori_loop(1, S, p2, 0)
    for j in range(1, H):
        def p3(k, _, j=j):
            tok = sec(-k) * T + ten(-j)
            landed(hbuf, ag_recv, tok)
            ag(tok, s, pt)
            return 0

        lax.fori_loop(0, S, p3, 0)

    tgt_copy.wait()
    lg_copy.wait()
    tcol = lax.fori_loop(
        0, n, lambda i, x: jnp.where(lax.broadcasted_iota(jnp.int32, (n, LANES), 0) == i, tgt_ref[i], x),
        jnp.zeros((n, LANES), jnp.int32))[:, :1]

    for j in range(H):
        def p4(k, _, j=j):
            tok = sec(-k) * T + lax.rem(pt + 2 * j, T)
            landed(hbuf, ag_recv, tok)
            return 0

        lax.fori_loop(0, S, p4, 0)

    def widen(i, _):
        slab[pl.ds(pl.multiple_of(i * pitch, 8), C), :] = hbuf[i].astype(jnp.float32)
        return 0

    lax.fori_loop(0, n, widen, 0)
    for q in range(parts):
        w_copy(q).wait()

    KC = GROUP * LANES

    wide = math.gcd(C, WIDE)
    span = wide * LANES

    def dot1(kc, acc):
        lhs = jnp.concatenate(
            [slab[pl.ds(kc * wide + i, n, stride=pitch), :] for i in range(wide)], axis=1).astype(jnp.bfloat16)
        w = wv[:, pl.ds(pl.multiple_of(kc * span, span), span)]
        return acc + lax.dot_general(lhs, w, (((1,), (1,)), ((), ())), preferred_element_type=jnp.float32)

    logits = lax.fori_loop(0, D // span, dot1, jnp.zeros((n, V), jnp.float32))

    mask = lax.broadcasted_iota(jnp.int32, (n, V), 1) + me * V == tcol
    m = jnp.max(logits, axis=1, keepdims=True)
    e = jnp.exp(logits - m)
    total = jnp.sum(e, axis=1, keepdims=True)
    tl = jnp.sum(jnp.where(mask, logits, 0.0), axis=1, keepdims=True)
    ptl = jnp.sum(jnp.where(mask, e, 0.0), axis=1, keepdims=True)

    r = lax.broadcasted_iota(jnp.int32, (n, L), 0)
    c = lax.broadcasted_iota(jnp.int32, (n, L), 1)
    packed = jnp.where(c == r, m, jnp.where(c == r + n, total, jnp.where(c == r + 2 * n, tl, 0.0)))
    packed = jnp.sum(packed, axis=0, keepdims=True)
    st_send[0] = packed
    st_recv[0] = packed

    def share(k, _):
        o = lax.rem(me + k, n)
        pltpu.make_async_remote_copy(
            src_ref=st_send.at[0], dst_ref=st_recv.at[k], send_sem=st_ssem, recv_sem=st_rsem,
            device_id=(o // T, lax.rem(o, T)), device_id_type=MESH).start()
        return 0

    lax.fori_loop(1, n, share, 0)

    lhs2 = jnp.concatenate(
        [jnp.where(mask, 0.0, e), mask.astype(jnp.float32)], axis=0).astype(jnp.bfloat16)

    def dot2(kc, _):
        cols = pl.ds(pl.multiple_of(kc * KC, KC), KC)
        gt[:, cols] = jnp.dot(lhs2, wv[:, cols], preferred_element_type=jnp.float32)
        return 0

    lax.fori_loop(0, D // KC, dot2, 0)

    others = st_recv.at[pl.ds(1, n - 1)]
    pltpu.make_async_copy(others, others, st_rsem).wait()

    lane = lax.broadcasted_iota(jnp.int32, (1, L), 1)
    live = lane < n
    got_stats = st_recv[...]
    top = jnp.where(live, jnp.max(got_stats, axis=0), 0.0)
    gap = jnp.where(live[None], got_stats - top[None], 0.0)
    z = jnp.sum(jnp.exp(gap) * pltpu.roll(got_stats, L - n, 2), axis=0)
    g = pltpu.roll(jnp.sum(got_stats, axis=0), L - 2 * n, 1)
    z = jnp.where(live, z, 1.0)
    loss_ref[0] = jnp.sum(jnp.where(lane == me, top + jnp.log(z) - g, 0.0))
    top_c = jnp.sum(jnp.where(c == r, top, 0.0), axis=1, keepdims=True)
    z_c = jnp.sum(jnp.where(c == r, z, 0.0), axis=1, keepdims=True)
    scale = jnp.exp(m - top_c) / z_c
    hit = ptl * scale - 1.0

    def spread(kc, _):
        for i in range(GROUP):
            cols = pl.ds(pl.multiple_of(kc * KC + i * LANES, LANES), LANES)
            slab[pl.ds(kc * GROUP + i, n, stride=pitch), :] = scale * gt[:n, cols] + hit * gt[n:, cols]
        return 0

    lax.fori_loop(0, D // KC, spread, 0)

    def part(tok):
        return slab[pl.ds(pl.multiple_of(tok * pitch, 8), C), :]

    def rs(tok, slot, value, ds, dt):
        sendbuf[tok] = value.astype(jnp.bfloat16)
        pltpu.make_async_remote_copy(
            src_ref=sendbuf.at[tok], dst_ref=rbuf.at[slot], send_sem=rs_send,
            recv_sem=rs_recv.at[slot], device_id=(ds, dt), device_id_type=MESH).start()

    def got(slot):
        landed(rbuf, rs_recv, slot)
        return rbuf[slot].astype(jnp.float32)

    for j in [*range(1, H), 0]:
        def qa(k, _, j=j):
            tok = sec(k + 1) * T + lax.rem(pt + 2 * j, T)
            rs(tok, tok, part(tok), s, pt)
            return 0

        lax.fori_loop(0, S, qa, 0)

    for j in range(1, H):
        def qb(k, _, j=j):
            tp = ten(j)
            sp = sec(k + 1)
            tok = sp * T + tp
            rs(tok, sp * T + pt, part(tok) + got(tok), s, tp)
            return 0

        lax.fori_loop(0, S, qb, 0)

    def joined(sp):
        tok = sp * T + t
        acc = part(tok) + got(tok)
        for j in range(1, H):
            acc = acc + got(sp * T + lax.rem(pt + 2 * j, T))
        return acc

    def qc(k, _):
        sp = sec(k)
        rs(sp * T + t, s * T + pt, joined(sp), sp, t)
        return 0

    lax.fori_loop(1, S, qc, 0)
    mine = lax.fori_loop(1, S, lambda k, x: x + got(sec(-k) * T + pt), joined(s))
    out_ref[...] = (lg_ref[0] * mine).astype(jnp.bfloat16)

    sent = hbuf.at[pl.ds(0, n - 1)]
    pltpu.make_async_copy(sent, sent, ag_send).wait()
    pltpu.make_async_copy(others, others, st_ssem).wait()
    sent = sendbuf.at[pl.ds(0, n - 1)]
    pltpu.make_async_copy(sent, sent, rs_send).wait()


def solution(mesh):
    S, T = mesh.shape["section"], mesh.shape["tensor"]
    n = S * T

    def step(hidden, weight, targets, loss_grad):
        V, D = weight.shape
        C = D // LANES
        L = -(-3 * n // LANES) * LANES
        vmem, smem = pltpu.VMEM, pltpu.SMEM
        loss, grad = pl.pallas_call(
            functools.partial(kernel, S, T),
            out_shape=(
                jax.ShapeDtypeStruct((1,), jnp.float32),
                jax.ShapeDtypeStruct((C, LANES), jnp.bfloat16),
            ),
            in_specs=[
                pl.BlockSpec(memory_space=pl.ANY)
            ] * 4,
            out_specs=(pl.BlockSpec(memory_space=smem), pl.BlockSpec(memory_space=vmem)),
            scratch_shapes=[
                vmem((1, D), jnp.bfloat16),
                smem((n,), jnp.int32),
                smem((1,), jnp.float32),
                pltpu.SemaphoreType.DMA((3,)),
                vmem((V, D), jnp.bfloat16),
                vmem((n, C, LANES), jnp.bfloat16),
                vmem((n * (C + 8), LANES), jnp.float32),
                vmem((2 * n, D), jnp.float32),
                vmem((n, C, LANES), jnp.bfloat16),
                vmem((n, C, LANES), jnp.bfloat16),
                vmem((C, LANES), jnp.float32),
                vmem((1, 1, L), jnp.float32),
                vmem((n, 1, L), jnp.float32),
                pltpu.SemaphoreType.DMA((4,)),
                pltpu.SemaphoreType.DMA,
                pltpu.SemaphoreType.DMA((n,)),
                pltpu.SemaphoreType.DMA,
                pltpu.SemaphoreType.DMA,
                pltpu.SemaphoreType.DMA,
                pltpu.SemaphoreType.DMA((n,)),
            ],
            compiler_params=pltpu.CompilerParams(
                collective_id=0, has_side_effects=True, vmem_limit_bytes=67043328
            ),
        )(hidden, weight, targets, loss_grad)
        return loss, grad.reshape(1, D)

    return jax.shard_map(
        step,
        mesh=mesh,
        in_specs=(
            P(("section", "tensor"), None),
            P(("section", "tensor"), None),
            P(),
            P(("section", "tensor")),
        ),
        out_specs=(P(("section", "tensor")), P(("section", "tensor"), None)),
        check_vma=False,
    )
```
